32 devices in a mesh: wide: 8 (over z, x), narrow: 4 (over y, core).
Axes of the slice: x: 2, y: 2, z: 4, core: 2. Of those that a mesh axis runs over, the one named last changes fastest.
Arguments:
- tokens: bfloat16 [24, 4, 256, 768], P('wide', 'narrow'), may hold values from -6 to 6
- condition: bfloat16 [24, 768], P('wide'), may hold values from -6 to 6
- counts: int32 [8], P('wide'), may hold values from 1 to 3, as said below
- w_mod: bfloat16 [768, 4608], replicated, may hold values from -0.21875 to 0.21875
- w_qkv: bfloat16 [768, 2304], replicated, may hold values from -0.21875 to 0.21875
- w_out: bfloat16 [768, 768], replicated, may hold values from -1.75 to 1.75
- w_up: bfloat16 [768, 3072], replicated, may hold values from -0.21875 to 0.21875
- w_down: bfloat16 [3072, 768], replicated, may hold values from -0.109375 to 0.109375
- conv_attn: bfloat16 [768, 9], replicated, may hold values from -2 to 2
- conv_ffn: bfloat16 [3072, 9], replicated, may hold values from -2 to 2
- cotangent: bfloat16 [24, 4, 256, 768], P('wide', 'narrow'), may hold values from -6 to 6
Outputs:
- output: bfloat16 [24, 4, 256, 768], P('wide', 'narrow')
- token_grad: bfloat16 [24, 4, 256, 768], P('wide', 'narrow')
- cond_grad: float32 [24, 768], P('wide')
- mod_grad: float32 [768, 4608], P(('wide', 'narrow'))
- qkv_grad: float32 [768, 2304], P(('wide', 'narrow'))
- proj_grad: float32 [768, 768], P(('wide', 'narrow'))
- up_grad: float32 [768, 3072], P(('wide', 'narrow'))
- down_grad: float32 [3072, 768], P(('wide', 'narrow'))
- conv_attn_grad: float32 [768, 9], P(('wide', 'narrow'))
- conv_ffn_grad: float32 [3072, 9], P(('wide', 'narrow'))
The draws below stay inside these ranges and needn't reach their ends.
Inputs may be any that keep to these rules, and one draw needn't show every extreme that they name: `counts`: items with index b mod 3 at or above the count of their index of wide are padding; some index of wide holds 3 live items.
All inputs are finite; a program needn't handle non-finite values.
Results may differ from the reference program's by a relative error of at most 0.017.
The reference program's roundings to bfloat16 on the way count: a program that leaves them out, or rounds other values in their place, can miss the bound.
Values may be sent and summed in bfloat16 or wider, within the bound.
A program may use at most 192 MiB of HBM per device.

```python
from functools import partial
import jax
import jax.numpy as jnp
from jax import lax

D = 768
HEADS = 12
HEAD_DIM = 64
FF = 3072
SIDE = 32
ITEMS_DEV = 3
ITEMS = 24
QUAD = 256
N_WIDE = 8


def draw_counts(key, part):
    first_key, second_key = jax.random.split(jax.random.fold_in(key, 11))
    drawn = jax.random.randint(first_key, (N_WIDE,), 1, ITEMS_DEV + 1)
    chosen = jax.random.randint(second_key, (), 0, N_WIDE)
    return jnp.where(jnp.arange(N_WIDE, dtype=jnp.int32) == chosen, ITEMS_DEV, drawn).astype(jnp.int32)


def block_levels(key, dims, cuts, least, high):
    def one(axis_at, blocks):
        steps = jax.random.uniform(jax.random.fold_in(jax.random.fold_in(key, 6), axis_at), (blocks,), jnp.float32, least / len(cuts), high / len(cuts))
        return jnp.repeat(jnp.exp(steps), dims[axis_at] // blocks).reshape((-1,) + (1,) * (len(dims) - axis_at - 1))

    gain = one(*cuts[0])
    for cut in cuts[1:]:
        gain = gain * one(*cut)
    return gain


def bell_draw(key, shape, width, reach, cuts=(), held_as=jnp.bfloat16):
    gain = block_levels(key, shape, cuts, -0.22, 0.18) if cuts else 1.0
    values = jax.random.normal(key, shape, jnp.float32) * width * gain
    return jnp.minimum(jnp.maximum(values, -reach), reach).astype(held_as)


def setup_inputs(seed: int = 0) -> dict:
    key_list = jax.random.split(jax.random.key(seed), 12)
    return {
        "tokens": bell_draw(key_list[0], (ITEMS, 4, QUAD, D), 1.0, 6.0, ((0, 8), (1, 4))),
        "condition": bell_draw(key_list[1], (ITEMS, D), 1.0, 6.0, ((0, 8),)),
        "counts": draw_counts(jax.random.fold_in(key_list[11], 71), 0),
        "w_mod": bell_draw(key_list[3], (D, 6 * D), D ** -0.5, 0.21875),
        "w_qkv": bell_draw(key_list[4], (D, 3 * D), D ** -0.5, 0.21875),
        "w_out": bell_draw(key_list[5], (D, D), (D // 64) ** -0.5, 1.75),
        "w_up": bell_draw(key_list[6], (D, FF), D ** -0.5, 0.21875),
        "w_down": bell_draw(key_list[7], (FF, D), FF ** -0.5, 0.109375),
        "conv_attn": bell_draw(key_list[8], (D, 9), 9 ** -0.5, 2.0),
        "conv_ffn": bell_draw(key_list[9], (FF, 9), 9 ** -0.5, 2.0),
        "cotangent": bell_draw(key_list[10], (ITEMS, 4, QUAD, D), 1.0, 6.0, ((0, 8), (1, 4))),
    }


@jax.custom_vjp
def low(v):
    return lax.optimization_barrier(v.astype(jnp.bfloat16)).astype(jnp.float32)

@jax.custom_vjp
def low_back(v):
    return v

def low_keep(v):
    return (low(v), None)

def low_pass(kept, grad):
    return (grad,)

def back_keep(v):
    return (v, None)

def back_low(kept, grad):
    return (low(grad),)
low.defvjp(low_keep, low_pass)
low_back.defvjp(back_keep, back_low)
epsilon = 1e-06

def product(left, right):
    return jnp.dot(left, right, precision=lax.Precision.HIGHEST, preferred_element_type=jnp.float32)

def normed(field_map):
    average = lax.optimization_barrier(jnp.mean(field_map, -1, keepdims=True))
    centred = field_map - average
    variance = lax.optimization_barrier(jnp.mean(centred * centred, -1, keepdims=True))
    return centred * lax.rsqrt(variance + epsilon)

def depthwise(field_map, kernel):
    side_len = field_map.shape[1]
    padded = jnp.pad(field_map, ((0, 0), (1, 1), (1, 1), (0, 0)))
    summed = jnp.zeros(field_map.shape, jnp.float32)
    for stencil in range(9):
        row_off = stencil // 3
        col_off = stencil % 3
        summed = summed + padded[:, row_off:row_off + side_len, col_off:col_off + side_len] * kernel[:, stencil]
    return summed

def to_map(block):
    count = block.shape[0]
    half_side = SIDE // 2
    return block.reshape(count, 2, 2, half_side, half_side, -1).transpose(0, 1, 3, 2, 4, 5).reshape(count, SIDE, SIDE, -1)

def from_map(field_map):
    count = field_map.shape[0]
    half_side = SIDE // 2
    return field_map.reshape(count, 2, half_side, 2, half_side, -1).transpose(0, 1, 3, 2, 4, 5).reshape(count, 4, QUAD, -1)

def to_groups(field_map):
    count = field_map.shape[0]
    half_side = SIDE // 2
    return field_map.reshape(count, half_side, 2, half_side, 2, -1).transpose(0, 2, 4, 1, 3, 5).reshape(count, 4, QUAD, -1)

def from_groups(groups):
    count = groups.shape[0]
    half_side = SIDE // 2
    return groups.reshape(count, 2, 2, half_side, half_side, -1).transpose(0, 3, 1, 4, 2, 5).reshape(count, SIDE, SIDE, -1)

def layer_block(weights, inputs):
    w_mod, w_qkv, w_out, w_up, w_down, conv_attn, conv_ffn = weights
    block, cond_block, living = inputs
    count = block.shape[0]
    start_map = to_map(block)
    lifted = low(jax.nn.silu(cond_block))
    modulation = product(lifted, w_mod).reshape(count, 6, D)
    pieces = [modulation[:, place][:, None, None, :] for place in range(6)]
    first_in = low_back(low(normed(start_map) * (1.0 + pieces[1]) + pieces[0]))
    mixed_map = low_back(low(depthwise(first_in, conv_attn)))
    groups = to_groups(mixed_map)
    triple = low_back(low(product(groups, w_qkv))).reshape(count, 4, QUAD, 3, HEADS, HEAD_DIM)
    queries = triple[:, :, :, 0]
    key_rows = triple[:, :, :, 1]
    values = triple[:, :, :, 2]
    scores = jnp.einsum('bgqhe,bgkhe->bghqk', queries, key_rows, precision=lax.Precision.HIGHEST) * HEAD_DIM ** (-0.5)
    scores = low_back(scores)
    attn_probs = low(jax.nn.softmax(scores, axis=-1))
    attended = jnp.einsum('bghqk,bgkhe->bgqhe', attn_probs, values, precision=lax.Precision.HIGHEST)
    attended = low_back(low(attended.reshape(count, 4, QUAD, D)))
    branch = low_back(product(from_groups(attended), w_out))
    hidden_one = start_map + pieces[2] * branch
    second = low(normed(hidden_one) * (1.0 + pieces[4]) + pieces[3])
    raised = low_back(low(product(second, w_up)))
    filtered = low_back(depthwise(raised, conv_ffn))
    activated = low(jax.nn.gelu(filtered, approximate=True))
    branch_two = low_back(product(activated, w_down))
    result = (hidden_one + pieces[5] * branch_two) * living[:, None, None, None]
    return from_map(result)

def forward(weights, tokens_f, cond_f, living):
    blocks = ITEMS // ITEMS_DEV
    inputs = (tokens_f.reshape(blocks, ITEMS_DEV, 4, QUAD, D), cond_f.reshape(blocks, ITEMS_DEV, D), living.reshape(blocks, ITEMS_DEV))
    runner = jax.checkpoint(partial(layer_block, weights))
    return lax.map(runner, inputs).reshape(ITEMS, 4, QUAD, D)

def reference(tokens, condition, counts, w_mod, w_qkv, w_out, w_up, w_down, conv_attn, conv_ffn, cotangent):
    living = (jnp.arange(ITEMS_DEV, dtype=jnp.int32)[None, :] < counts[:, None]).astype(jnp.float32).reshape(ITEMS)
    weights = tuple((matrix.astype(jnp.float32) for matrix in (w_mod, w_qkv, w_out, w_up, w_down, conv_attn, conv_ffn)))

    def wrapped(weight_set, tokens_f, cond_f):
        return forward(weight_set, tokens_f, cond_f, living)
    output, pull = jax.vjp(wrapped, weights, tokens.astype(jnp.float32), condition.astype(jnp.float32))
    weight_grads, token_grad, cond_grad = pull(cotangent.astype(jnp.float32))
    return (output.astype(jnp.bfloat16), token_grad.astype(jnp.bfloat16), cond_grad, weight_grads[0], weight_grads[1], weight_grads[2], weight_grads[3], weight_grads[4], weight_grads[5], weight_grads[6])
```

```python
import math

import jax
import jax.numpy as jnp
from jax import lax
from jax.sharding import PartitionSpec as P

HEADS = 12
HEAD_DIM = 64


epsilon = 1e-06


def from_partner(shard, axis, bit):
    return lax.ppermute(shard, axis, [(i, i ^ 1 << bit) for i in range(lax.axis_size(axis))])


def normed(field_map):
    average = jnp.mean(field_map, -1, keepdims=True)
    centred = field_map - average
    variance = jnp.mean(centred * centred, -1, keepdims=True)
    return centred * lax.rsqrt(variance + epsilon)


def modulate(field_map, shift, scale):
    return normed(field_map) * (1.0 + scale) + shift


def gelu_tanh(field_map):
    return jax.nn.gelu(field_map, approximate=True)


def attn_across(outgoing):
    return from_partner(outgoing, "narrow", 0)


def attn_down(outgoing):
    return from_partner(outgoing, "narrow", 1)


def ffn_across(outgoing):
    return from_partner(outgoing, "narrow", 0)


def ffn_down(outgoing):
    return from_partner(outgoing, "narrow", 1)


def extend(field_map, row_half, col_half, across, down):
    outgoing = jnp.where(col_half == 0, field_map[:, :, -1:], field_map[:, :, :1])
    incoming = across(outgoing)
    zeros_rim = jnp.zeros_like(incoming)
    left_rim = jnp.where(col_half == 1, incoming, zeros_rim)
    right_rim = jnp.where(col_half == 0, incoming, zeros_rim)
    widened = jnp.concatenate([left_rim, field_map, right_rim], 2)
    outgoing = jnp.where(row_half == 0, widened[:, -1:], widened[:, :1])
    incoming = down(outgoing)
    zeros_rim = jnp.zeros_like(incoming)
    top_rim = jnp.where(row_half == 1, incoming, zeros_rim)
    bottom_rim = jnp.where(row_half == 0, incoming, zeros_rim)
    return jnp.concatenate([top_rim, widened, bottom_rim], 1)


def apply_taps(padded, kernel, side_len, flipped):
    summed = jnp.zeros((padded.shape[0], side_len, side_len, padded.shape[3]), jnp.float32)
    weights_f = kernel.astype(jnp.float32)
    for stencil in range(9):
        row_off = stencil // 3
        col_off = stencil % 3
        if flipped:
            row_off = 2 - row_off
            col_off = 2 - col_off
        window = padded[:, row_off : row_off + side_len, col_off : col_off + side_len].astype(
            jnp.float32
        )
        summed = summed + window * weights_f[:, stencil]
    return summed


def tap_grads(padded, grad_map, side_len):
    grad_f = grad_map.astype(jnp.float32)
    columns = []
    for stencil in range(9):
        row_off = stencil // 3
        col_off = stencil % 3
        window = padded[:, row_off : row_off + side_len, col_off : col_off + side_len].astype(
            jnp.float32
        )
        columns.append(jnp.sum(window * grad_f, axis=(0, 1, 2)))
    return jnp.stack(columns, 1)


def to_groups(field_map):
    count, side_len, _, channels = field_map.shape
    quarter = side_len // 2
    pieces = field_map.reshape(count, quarter, 2, quarter, 2, channels).transpose(0, 2, 4, 1, 3, 5)
    pieces = pieces.reshape(count, 4, quarter * quarter, channels)
    incoming = lax.all_to_all(pieces, "narrow", split_axis=1, concat_axis=1, tiled=True)
    return incoming.reshape(count, 4 * quarter * quarter, channels)


def to_quads(group_rows):
    count, rows_all, channels = group_rows.shape
    pieces = group_rows.reshape(count, 4, rows_all // 4, channels)
    incoming = lax.all_to_all(pieces, "narrow", split_axis=1, concat_axis=1, tiled=True)
    quarter = math.isqrt(rows_all // 4)
    incoming = incoming.reshape(count, 2, 2, quarter, quarter, channels).transpose(0, 3, 1, 4, 2, 5)
    return incoming.reshape(count, 2 * quarter, 2 * quarter, channels)


def split_heads(groups, w_qkv):
    count, rows_all, _ = groups.shape
    triple = jnp.dot(groups, w_qkv, preferred_element_type=jnp.float32).astype(jnp.bfloat16)
    triple = triple.reshape(count, rows_all, 3, HEADS, HEAD_DIM)
    return (triple[:, :, 0], triple[:, :, 1], triple[:, :, 2])


def score(queries, key_rows):
    return jnp.einsum(
        "iqhe,ikhe->ihqk", queries, key_rows, preferred_element_type=jnp.float32
    ) * HEAD_DIM ** (-0.5)


def narrow_sum(part):
    for bit in range(lax.axis_size("narrow").bit_length() - 1):
        part = part + from_partner(part, "narrow", bit)
    return part


def wide_gather(block):
    count = lax.axis_size("wide")
    place = lax.axis_index("wide")
    held = block[None]
    for bit in range(count.bit_length() - 1):
        other = from_partner(held, "wide", bit)
        mine_high = (place >> bit) & 1
        low = jnp.where(mine_high == 1, other, held)
        high = jnp.where(mine_high == 1, held, other)
        held = jnp.concatenate([low, high], 0)
    return held.reshape((count * block.shape[0],) + block.shape[1:])


def split_dot(exact, coarse, dims):
    high = exact.astype(jnp.bfloat16)
    low = (exact - high.astype(jnp.float32)).astype(jnp.bfloat16)
    high_dot = lax.dot_general(high, coarse, (dims, ((), ())), preferred_element_type=jnp.float32)
    low_dot = lax.dot_general(low, coarse, (dims, ((), ())), preferred_element_type=jnp.float32)
    return high_dot + low_dot


def halving_sum(blocks, colour):
    wide_bits = lax.axis_size("wide").bit_length() - 1
    narrow_bits = lax.axis_size("narrow").bit_length() - 1
    order = [("narrow", 0)]
    first = [("wide", 0), ("narrow", 1)]
    order += first if colour == 0 else first[::-1]
    order += [("wide", bit) for bit in range(1, wide_bits)]
    names = [("wide", bit) for bit in range(wide_bits - 1, -1, -1)]
    names += [("narrow", bit) for bit in range(narrow_bits - 1, -1, -1)]
    held = blocks.reshape((2,) * len(names) + blocks.shape[1:])
    for step, (axis, bit) in enumerate(order):
        where = names.index((axis, bit))
        names.pop(where)
        mine = (lax.axis_index(axis) >> bit) & 1
        keep = lax.dynamic_index_in_dim(held, mine, where, keepdims=False)
        give = lax.dynamic_index_in_dim(held, 1 - mine, where, keepdims=False)
        got = from_partner(give, axis, bit)
        held = keep.astype(jnp.float32) + got.astype(jnp.float32)
        if step < len(order) - 1:
            held = held.astype(jnp.bfloat16)
    return held


def shards(
    tokens, condition, counts, w_mod, w_qkv, w_out, w_up, w_down, conv_attn, conv_ffn, cotangent
):
    item_count, _, quad_rows, channels = tokens.shape
    half_side = math.isqrt(quad_rows)
    corner = lax.axis_index("narrow")
    row_half = corner // 2
    col_half = corner % 2
    living = (jnp.arange(item_count, dtype=jnp.int32) < counts[0]).astype(jnp.float32)[
        :, None, None, None
    ]
    start_map = tokens.reshape(item_count, half_side, half_side, channels).astype(jnp.float32)
    cond_f = condition.astype(jnp.float32)
    lifted = jax.nn.silu(cond_f).astype(jnp.bfloat16)
    all_lifted = wide_gather(lifted)
    modulation = jnp.dot(lifted, w_mod, preferred_element_type=jnp.float32).reshape(
        item_count, 6, channels
    )
    pieces = [modulation[:, place][:, None, None, :] for place in range(6)]
    shift_a, scale_a, gate_a, shift_f, scale_f, gate_f = pieces
    first_f, pull_attn_norm = jax.vjp(modulate, start_map, shift_a, scale_a)
    first_in = first_f.astype(jnp.bfloat16)
    padded_attn = extend(first_in, row_half, col_half, attn_across, attn_down)
    mixed_map = apply_taps(padded_attn, conv_attn, half_side, False).astype(jnp.bfloat16)
    groups = to_groups(mixed_map)
    queries, key_rows, values = split_heads(groups, w_qkv)
    scores = score(queries, key_rows)
    peak = jnp.max(scores, -1, keepdims=True)
    raised_exp = jnp.exp(scores - peak)
    summed = jnp.sum(raised_exp, -1, keepdims=True)
    attn_probs = (raised_exp / summed).astype(jnp.bfloat16)
    log_total = peak + jnp.log(summed)
    attended = jnp.einsum("ihqk,ikhe->iqhe", attn_probs, values, preferred_element_type=jnp.float32)
    attended = attended.astype(jnp.bfloat16).reshape(item_count, quad_rows, channels)
    returned = to_quads(attended)
    branch = jnp.dot(returned, w_out, preferred_element_type=jnp.float32)
    hidden_one = start_map + gate_a * branch
    second_f, pull_ffn_norm = jax.vjp(modulate, hidden_one, shift_f, scale_f)
    second = second_f.astype(jnp.bfloat16)
    raised = jnp.dot(second, w_up, preferred_element_type=jnp.float32).astype(jnp.bfloat16)
    padded_ffn = extend(raised, row_half, col_half, ffn_across, ffn_down)
    filtered = apply_taps(padded_ffn, conv_ffn, half_side, False)
    activated = gelu_tanh(filtered).astype(jnp.bfloat16)
    branch_two = jnp.dot(activated, w_down, preferred_element_type=jnp.float32)
    output = ((hidden_one + gate_f * branch_two) * living).astype(jnp.bfloat16)
    grad_res = (
        cotangent.reshape(item_count, half_side, half_side, channels).astype(jnp.float32) * living
    )
    d_gate_f = jnp.sum(grad_res * branch_two, (1, 2))
    d_branch_two = (grad_res * gate_f).astype(jnp.bfloat16)
    down_grad = jnp.einsum(
        "ixyf,ixyd->fd", activated, d_branch_two, preferred_element_type=jnp.float32
    )
    d_activated = jnp.einsum(
        "ixyd,fd->ixyf", d_branch_two, w_down, preferred_element_type=jnp.float32
    )
    again = jnp.dot(second, w_up, preferred_element_type=jnp.float32).astype(jnp.bfloat16)
    kept_pad = extend(again, row_half, col_half, ffn_across, ffn_down)
    kept_filter = apply_taps(kept_pad, conv_ffn, half_side, False)
    _, gelu_pull = jax.vjp(gelu_tanh, kept_filter)
    d_filtered = gelu_pull(d_activated)[0].astype(jnp.bfloat16)
    conv_ffn_grad = tap_grads(kept_pad, d_filtered, half_side)
    d_padded_ffn = extend(d_filtered, row_half, col_half, ffn_across, ffn_down)
    d_raised = apply_taps(d_padded_ffn, conv_ffn, half_side, True).astype(jnp.bfloat16)
    up_grad = jnp.einsum("ixyd,ixyf->df", second, d_raised, preferred_element_type=jnp.float32)
    d_second = jnp.einsum("ixyf,df->ixyd", d_raised, w_up, preferred_element_type=jnp.float32)
    d_hidden_part, d_shift_f, d_scale_f = pull_ffn_norm(d_second)
    d_hidden = grad_res + d_hidden_part
    d_gate_a = jnp.sum(d_hidden * branch, (1, 2))
    d_branch = (d_hidden * gate_a).astype(jnp.bfloat16)
    proj_grad = jnp.einsum("ixyd,ixye->de", returned, d_branch, preferred_element_type=jnp.float32)
    d_returned = jnp.einsum(
        "ixye,de->ixyd", d_branch, w_out, preferred_element_type=jnp.float32
    ).astype(jnp.bfloat16)
    d_attended = to_groups(d_returned).reshape(item_count, quad_rows, HEADS, HEAD_DIM)
    queries, key_rows, values = split_heads(groups, w_qkv)
    scores = score(queries, key_rows)
    exact = jnp.exp(scores - log_total)
    rounded = exact.astype(jnp.bfloat16)
    d_probs = jnp.einsum("iqhe,ikhe->ihqk", d_attended, values, preferred_element_type=jnp.float32)
    d_values = jnp.einsum(
        "ihqk,iqhe->ikhe", rounded, d_attended, preferred_element_type=jnp.float32
    )
    d_scores = (exact * (d_probs - jnp.sum(d_probs * exact, -1, keepdims=True))).astype(
        jnp.bfloat16
    )
    d_queries = jnp.einsum(
        "ihqk,ikhe->iqhe", d_scores, key_rows, preferred_element_type=jnp.float32
    ) * HEAD_DIM ** (-0.5)
    d_keys = jnp.einsum(
        "ihqk,iqhe->ikhe", d_scores, queries, preferred_element_type=jnp.float32
    ) * HEAD_DIM ** (-0.5)
    d_triple = (
        jnp.stack([d_queries, d_keys, d_values], 2)
        .astype(jnp.bfloat16)
        .reshape(item_count, quad_rows, 3 * channels)
    )
    qkv_grad = jnp.einsum("iqd,iqe->de", groups, d_triple, preferred_element_type=jnp.float32)
    d_groups = jnp.einsum(
        "iqe,de->iqd", d_triple, w_qkv, preferred_element_type=jnp.float32
    ).astype(jnp.bfloat16)
    d_mixed = to_quads(d_groups)
    conv_attn_grad = tap_grads(padded_attn, d_mixed, half_side)
    d_padded_attn = extend(d_mixed, row_half, col_half, attn_across, attn_down)
    d_first = apply_taps(d_padded_attn, conv_attn, half_side, True).astype(jnp.bfloat16)
    d_start, d_shift_a, d_scale_a = pull_attn_norm(d_first.astype(jnp.float32))
    token_grad = (d_hidden + d_start).astype(jnp.bfloat16).reshape(tokens.shape)
    flat_parts = [
        d_shift_a.reshape(item_count, channels),
        d_scale_a.reshape(item_count, channels),
        d_gate_a,
        d_shift_f.reshape(item_count, channels),
        d_scale_f.reshape(item_count, channels),
        d_gate_f,
    ]
    d_modulation = jnp.stack(flat_parts, 1).reshape(item_count, 6 * channels)
    d_modulation = narrow_sum(d_modulation)
    _, silu_pull = jax.vjp(jax.nn.silu, cond_f)
    d_lifted = split_dot(d_modulation, w_mod, ((1,), (1,)))
    cond_grad = silu_pull(d_lifted)[0]
    all_modulation = wide_gather(d_modulation)
    block_rows = channels // (lax.axis_size("wide") * lax.axis_size("narrow"))
    own_block = lax.axis_index("wide") * lax.axis_size("narrow") + corner
    own_lifted = lax.dynamic_slice_in_dim(all_lifted, own_block * block_rows, block_rows, 1)
    mod_sum = split_dot(all_modulation, own_lifted, ((0,), (0,))).T
    blocks = lax.axis_size("wide") * lax.axis_size("narrow")
    up_blocks = up_grad.astype(jnp.bfloat16).reshape(blocks, -1, up_grad.shape[1])
    down_blocks = down_grad.astype(jnp.bfloat16).reshape(blocks, -1, channels)
    up_sum = halving_sum(up_blocks, 0)
    down_sum = halving_sum(down_blocks, 1)
    qkv_blocks = qkv_grad.astype(jnp.bfloat16).reshape(blocks, -1, 3 * channels)
    proj_blocks = proj_grad.astype(jnp.bfloat16).reshape(blocks, -1, channels)
    taps = jnp.concatenate([conv_attn_grad.reshape(blocks, -1), conv_ffn_grad.reshape(blocks, -1)], 1)
    rows = qkv_blocks.shape[1]
    taps_len = taps.shape[1]
    taps_wide = -(-taps_len // (rows * 128)) * 128
    taps = jnp.pad(taps, ((0, 0), (0, rows * taps_wide - taps_len)))
    taps = taps.astype(jnp.bfloat16).reshape(blocks, rows, taps_wide)
    left_sum = halving_sum(qkv_blocks[:, :, : 2 * channels], 0)
    right = jnp.concatenate([qkv_blocks[:, :, 2 * channels :], proj_blocks, taps], 2)
    right_sum = halving_sum(right, 1)
    qkv_sum = jnp.concatenate([left_sum, right_sum[:, :channels]], 1)
    proj_sum = right_sum[:, channels : 2 * channels]
    tap_sums = right_sum[:, 2 * channels :].reshape(-1)
    attn_len = conv_attn_grad.size // blocks
    conv_attn_sum = tap_sums[:attn_len].reshape(-1, 9)
    conv_ffn_sum = tap_sums[attn_len:taps_len].reshape(-1, 9)
    return (
        output.reshape(tokens.shape),
        token_grad,
        cond_grad,
        mod_sum,
        qkv_sum,
        proj_sum,
        up_sum,
        down_sum,
        conv_attn_sum,
        conv_ffn_sum,
    )


def solution(mesh):
    in_specs = (
        P("wide", "narrow", None, None),
        P("wide", None),
        P("wide"),
        P(),
        P(),
        P(),
        P(),
        P(),
        P(),
        P(),
        P("wide", "narrow", None, None),
    )
    out_specs = (
        P("wide", "narrow", None, None),
        P("wide", "narrow", None, None),
        P("wide", None),
        P(("wide", "narrow"), None),
        P(("wide", "narrow"), None),
        P(("wide", "narrow"), None),
        P(("wide", "narrow"), None),
        P(("wide", "narrow"), None),
        P(("wide", "narrow"), None),
        P(("wide", "narrow"), None),
    )
    return jax.shard_map(shards, mesh=mesh, in_specs=in_specs, out_specs=out_specs, check_vma=False)
```

```python
import functools
import math

import jax
import jax.numpy as jnp
from jax import lax
from jax.experimental import pallas as pl
from jax.experimental.pallas import tpu as pltpu
from jax.sharding import PartitionSpec as P

HEADS = 12
HEAD_DIM = 64


epsilon = 1e-06


def from_partner(shard, axis, bit):
    return lax.ppermute(shard, axis, [(i, i ^ 1 << bit) for i in range(lax.axis_size(axis))])


def normed(field_map):
    average = jnp.mean(field_map, -1, keepdims=True)
    centred = field_map - average
    variance = jnp.mean(centred * centred, -1, keepdims=True)
    return centred * lax.rsqrt(variance + epsilon)


def modulate(field_map, shift, scale):
    return normed(field_map) * (1.0 + scale) + shift


def attn_across(outgoing):
    return from_partner(outgoing, "narrow", 0)


def attn_down(outgoing):
    return from_partner(outgoing, "narrow", 1)


def extend(field_map, row_half, col_half, across, down):
    outgoing = jnp.where(col_half == 0, field_map[:, :, -1:], field_map[:, :, :1])
    incoming = across(outgoing)
    zeros_rim = jnp.zeros_like(incoming)
    left_rim = jnp.where(col_half == 1, incoming, zeros_rim)
    right_rim = jnp.where(col_half == 0, incoming, zeros_rim)
    widened = jnp.concatenate([left_rim, field_map, right_rim], 2)
    outgoing = jnp.where(row_half == 0, widened[:, -1:], widened[:, :1])
    incoming = down(outgoing)
    zeros_rim = jnp.zeros_like(incoming)
    top_rim = jnp.where(row_half == 1, incoming, zeros_rim)
    bottom_rim = jnp.where(row_half == 0, incoming, zeros_rim)
    return jnp.concatenate([top_rim, widened, bottom_rim], 1)


def apply_taps(padded, kernel, side_len, flipped):
    summed = jnp.zeros((padded.shape[0], side_len, side_len, padded.shape[3]), jnp.float32)
    weights_f = kernel.astype(jnp.float32)
    for stencil in range(9):
        row_off = stencil // 3
        col_off = stencil % 3
        if flipped:
            row_off = 2 - row_off
            col_off = 2 - col_off
        window = padded[:, row_off : row_off + side_len, col_off : col_off + side_len].astype(
            jnp.float32
        )
        summed = summed + window * weights_f[:, stencil]
    return summed


def tap_grads(padded, grad_map, side_len):
    grad_f = grad_map.astype(jnp.float32)
    columns = []
    for stencil in range(9):
        row_off = stencil // 3
        col_off = stencil % 3
        window = padded[:, row_off : row_off + side_len, col_off : col_off + side_len].astype(
            jnp.float32
        )
        columns.append(jnp.sum(window * grad_f, axis=(0, 1, 2)))
    return jnp.stack(columns, 1)


def to_groups(field_map):
    count, side_len, _, channels = field_map.shape
    quarter = side_len // 2
    pieces = field_map.reshape(count, quarter, 2, quarter, 2, channels).transpose(0, 2, 4, 1, 3, 5)
    pieces = pieces.reshape(count, 4, quarter * quarter, channels)
    incoming = lax.all_to_all(pieces, "narrow", split_axis=1, concat_axis=1, tiled=True)
    return incoming.reshape(count, 4 * quarter * quarter, channels)


def to_quads(group_rows):
    count, rows_all, channels = group_rows.shape
    pieces = group_rows.reshape(count, 4, rows_all // 4, channels)
    incoming = lax.all_to_all(pieces, "narrow", split_axis=1, concat_axis=1, tiled=True)
    quarter = math.isqrt(rows_all // 4)
    incoming = incoming.reshape(count, 2, 2, quarter, quarter, channels).transpose(0, 3, 1, 4, 2, 5)
    return incoming.reshape(count, 2 * quarter, 2 * quarter, channels)


def split_heads(groups, w_qkv):
    count, rows_all, _ = groups.shape
    triple = jnp.dot(groups, w_qkv, preferred_element_type=jnp.float32).astype(jnp.bfloat16)
    triple = triple.reshape(count, rows_all, 3, HEADS, HEAD_DIM)
    return (triple[:, :, 0], triple[:, :, 1], triple[:, :, 2])


def score(queries, key_rows):
    return jnp.einsum(
        "iqhe,ikhe->ihqk", queries, key_rows, preferred_element_type=jnp.float32
    ) * HEAD_DIM ** (-0.5)


def narrow_sum(part):
    for bit in range(lax.axis_size("narrow").bit_length() - 1):
        part = part + from_partner(part, "narrow", bit)
    return part


def wide_gather(block):
    count = lax.axis_size("wide")
    place = lax.axis_index("wide")
    held = block[None]
    for bit in range(count.bit_length() - 1):
        other = from_partner(held, "wide", bit)
        mine_high = (place >> bit) & 1
        low = jnp.where(mine_high == 1, other, held)
        high = jnp.where(mine_high == 1, held, other)
        held = jnp.concatenate([low, high], 0)
    return held.reshape((count * block.shape[0],) + block.shape[1:])


def split_dot(exact, coarse, dims):
    high = exact.astype(jnp.bfloat16)
    low = (exact - high.astype(jnp.float32)).astype(jnp.bfloat16)
    high_dot = lax.dot_general(high, coarse, (dims, ((), ())), preferred_element_type=jnp.float32)
    low_dot = lax.dot_general(low, coarse, (dims, ((), ())), preferred_element_type=jnp.float32)
    return high_dot + low_dot


def halving_sum(blocks, colour):
    wide_bits = lax.axis_size("wide").bit_length() - 1
    narrow_bits = lax.axis_size("narrow").bit_length() - 1
    order = [("narrow", 0)]
    first = [("wide", 0), ("narrow", 1)]
    order += first if colour == 0 else first[::-1]
    order += [("wide", bit) for bit in range(1, wide_bits)]
    names = [("wide", bit) for bit in range(wide_bits - 1, -1, -1)]
    names += [("narrow", bit) for bit in range(narrow_bits - 1, -1, -1)]
    held = blocks.reshape((2,) * len(names) + blocks.shape[1:])
    for step, (axis, bit) in enumerate(order):
        where = names.index((axis, bit))
        names.pop(where)
        mine = (lax.axis_index(axis) >> bit) & 1
        keep = lax.dynamic_index_in_dim(held, mine, where, keepdims=False)
        give = lax.dynamic_index_in_dim(held, 1 - mine, where, keepdims=False)
        got = from_partner(give, axis, bit)
        held = keep.astype(jnp.float32) + got.astype(jnp.float32)
        if step < len(order) - 1:
            held = held.astype(jnp.bfloat16)
    return held


LANES = 128
INSET = 8
GELU_SCALE = math.sqrt(2.0 / math.pi)
GELU_CUBE = 0.044715


def rim_exchange(field_map, row_half, col_half):
    column = jnp.where(col_half == 0, field_map[:, :, -1], field_map[:, :, 0])
    row = jnp.where(row_half == 0, field_map[:, -1], field_map[:, 0])
    point = jnp.where(col_half == 0, row[:, -1:], row[:, :1])
    size = lax.axis_size("narrow")
    column = lax.ppermute(column, "narrow", [(i, i ^ 1) for i in range(size)])
    row = lax.ppermute(row, "narrow", [(i, i ^ 2) for i in range(size)])
    point = lax.ppermute(point, "narrow", [(i, i ^ 3) for i in range(size)])
    upper = row_half == 1
    left = col_half == 1

    def kept(values, where):
        return jnp.where(where, values, jnp.zeros_like(values))

    spare = jnp.zeros((point.shape[0], 4) + point.shape[2:], point.dtype)
    return jnp.concatenate(
        [
            kept(column, left),
            kept(column, ~left),
            kept(row, upper),
            kept(row, ~upper),
            kept(point, upper & left),
            kept(point, upper & ~left),
            kept(point, ~upper & left),
            kept(point, ~upper & ~left),
            spare,
        ],
        1,
    )


def fill_padded(padded, inner, rim, items, side):
    high = side + 2
    area = side * side
    count = 4 * side + 8
    for item in range(items):
        top = item * high
        block = inner[item * area : (item + 1) * area]
        padded[top + 1 : top + 1 + side, INSET : INSET + side, :] = block.reshape(side, side, -1)
        base = item * count
        padded[top, INSET : INSET + side, :] = rim[base + 2 * side : base + 3 * side, :]
        padded[top + side + 1, INSET : INSET + side, :] = rim[base + 3 * side : base + 4 * side, :]
        for corner, (row, col) in enumerate(
            [(0, INSET - 1), (0, INSET + side), (side + 1, INSET - 1), (side + 1, INSET + side)]
        ):
            at = base + 4 * side + corner
            padded[top + row, col : col + 1, :] = rim[at : at + 1, :]
        for row in range(side):
            padded[top + 1 + row, INSET - 1 : INSET, :] = rim[base + row : base + row + 1, :]
            at = base + side + row
            padded[top + 1 + row, INSET + side : INSET + side + 1, :] = rim[at : at + 1, :]


def ffn_kernel(
    items,
    side,
    second_ref,
    rim_ref,
    d_two_ref,
    w_up_ref,
    w_down_ref,
    taps_ref,
    two_ref,
    d_filtered_ref,
    down_ref,
    tap_grad_ref,
    padded,
    rim,
    act,
    d_act,
):
    chunk = w_up_ref.shape[1]
    low = jnp.bfloat16
    raised = jnp.dot(second_ref[...], w_up_ref[...], preferred_element_type=jnp.float32)
    rim[...] = (
        jnp.dot(rim_ref[...], w_up_ref[...], preferred_element_type=jnp.float32)
        .astype(low)
        .astype(jnp.float32)
    )
    fill_padded(padded, raised.astype(low).astype(jnp.float32), rim, items, side)
    d_act[...] = lax.dot_general(
        d_two_ref[...], w_down_ref[...], (((1,), (1,)), ((), ())), preferred_element_type=jnp.float32
    )
    for lane in range(0, chunk, LANES):
        lanes = slice(lane, lane + LANES)
        weights = [taps_ref[tap : tap + 1, lanes] for tap in range(9)]
        sums = tuple(jnp.zeros((8, LANES), jnp.float32) for _ in range(9))
        for item in range(items):

            def one_row(row, sums, item=item):
                top = item * (side + 2) + row
                at = pl.ds(pl.multiple_of(item * side * side + row * side, side), side)
                windows = [
                    padded[top + tap // 3, INSET - 1 + tap % 3 : INSET - 1 + tap % 3 + side, lanes]
                    for tap in range(9)
                ]
                v = windows[0] * weights[0]
                for tap in range(1, 9):
                    v = v + windows[tap] * weights[tap]
                square = v * v
                bend = jnp.tanh(GELU_SCALE * v * (1.0 + GELU_CUBE * square))
                half = 0.5 + 0.5 * bend
                act[at, lanes] = (v * half).astype(low)
                slope = half + 0.5 * v * (1.0 - bend * bend) * (
                    GELU_SCALE + (3.0 * GELU_CUBE * GELU_SCALE) * square
                )
                rounded = (d_act[at, lanes] * slope).astype(low)
                d_filtered_ref[at, lanes] = rounded
                wide = rounded.astype(jnp.float32)
                added = []
                for tap in range(9):
                    product = windows[tap] * wide
                    total = sums[tap]
                    for part in range(0, side, 8):
                        total = total + product[part : part + 8]
                    added.append(total)
                return tuple(added)

            sums = lax.fori_loop(0, side, one_row, sums)
        for tap in range(9):
            tap_grad_ref[tap : tap + 1, lanes] = jnp.sum(sums[tap], 0, keepdims=True)
    tap_grad_ref[9:, :] = jnp.zeros((tap_grad_ref.shape[0] - 9, chunk), jnp.float32)
    down_ref[...] = lax.dot_general(
        act[...], d_two_ref[...], (((0,), (0,)), ((), ())), preferred_element_type=jnp.float32
    ).astype(low)
    part_two = jnp.dot(act[...], w_down_ref[...], preferred_element_type=jnp.float32)

    @pl.when(pl.program_id(0) == 0)
    def _():
        two_ref[...] = part_two

    @pl.when(pl.program_id(0) > 0)
    def _():
        two_ref[...] += part_two


def ffn_back_kernel(
    items,
    side,
    d_filtered_ref,
    rim_ref,
    flipped_ref,
    w_up_ref,
    taps_ref,
    up_ref,
    d_second_ref,
    padded,
    rim,
    d_raised,
):
    chunk = w_up_ref.shape[1]
    low = jnp.bfloat16
    rim[...] = rim_ref[...].astype(jnp.float32)
    fill_padded(padded, d_filtered_ref[...].astype(jnp.float32), rim, items, side)
    for lane in range(0, chunk, LANES):
        lanes = slice(lane, lane + LANES)
        weights = [taps_ref[8 - tap : 9 - tap, lanes] for tap in range(9)]
        for item in range(items):

            def one_row(row, carry, item=item):
                top = item * (side + 2) + row
                at = pl.ds(pl.multiple_of(item * side * side + row * side, side), side)
                v = None
                for tap in range(9):
                    first = INSET - 1 + tap % 3
                    term = padded[top + tap // 3, first : first + side, lanes] * weights[tap]
                    v = term if v is None else v + term
                d_raised[at, lanes] = v.astype(low)
                return carry

            lax.fori_loop(0, side, one_row, 0)
    up_ref[...] = jnp.dot(
        flipped_ref[...], d_raised[...], preferred_element_type=jnp.float32
    ).astype(low)
    part = lax.dot_general(
        d_raised[...], w_up_ref[...], (((1,), (1,)), ((), ())), preferred_element_type=jnp.float32
    )

    @pl.when(pl.program_id(0) == 0)
    def _():
        d_second_ref[...] = part

    @pl.when(pl.program_id(0) > 0)
    def _():
        d_second_ref[...] += part


def ffn_pass(second, rim, d_two, w_up, w_down, taps, items, side, chunk=256):
    tokens, channels = second.shape
    wide = w_up.shape[1]
    rims = rim.shape[0]
    fixed = lambda step: (0, 0)
    columns = lambda step: (0, step)
    rows = lambda step: (step, 0)
    return pl.pallas_call(
        functools.partial(ffn_kernel, items, side),
        grid=(wide // chunk,),
        in_specs=[
            pl.BlockSpec((tokens, channels), fixed),
            pl.BlockSpec((rims, channels), fixed),
            pl.BlockSpec((tokens, channels), fixed),
            pl.BlockSpec((channels, chunk), columns),
            pl.BlockSpec((chunk, channels), rows),
            pl.BlockSpec((16, chunk), columns),
        ],
        out_specs=[
            pl.BlockSpec((tokens, channels), fixed),
            pl.BlockSpec((tokens, chunk), columns),
            pl.BlockSpec((chunk, channels), rows),
            pl.BlockSpec((16, chunk), columns),
        ],
        out_shape=[
            jax.ShapeDtypeStruct((tokens, channels), jnp.float32),
            jax.ShapeDtypeStruct((tokens, wide), jnp.bfloat16),
            jax.ShapeDtypeStruct((wide, channels), jnp.bfloat16),
            jax.ShapeDtypeStruct((16, wide), jnp.float32),
        ],
        scratch_shapes=[
            pltpu.VMEM((items * (side + 2), side + 2 * INSET, chunk), jnp.float32),
            pltpu.VMEM((rims, chunk), jnp.float32),
            pltpu.VMEM((tokens, chunk), jnp.bfloat16),
            pltpu.VMEM((tokens, chunk), jnp.float32),
        ],
        cost_estimate=pl.CostEstimate(
            flops=8 * tokens * channels * wide,
            bytes_accessed=4 * channels * wide * 4,
            transcendentals=tokens * wide,
        ),
        name="ffn",
    )(second, rim, d_two, w_up, w_down, taps)


def ffn_back_pass(d_filtered, rim, flipped, w_up, taps, items, side, chunk=256):
    tokens, wide = d_filtered.shape
    channels = w_up.shape[0]
    rims = rim.shape[0]
    fixed = lambda step: (0, 0)
    columns = lambda step: (0, step)
    return pl.pallas_call(
        functools.partial(ffn_back_kernel, items, side),
        grid=(wide // chunk,),
        in_specs=[
            pl.BlockSpec((tokens, chunk), columns),
            pl.BlockSpec((rims, chunk), columns),
            pl.BlockSpec((channels, tokens), fixed),
            pl.BlockSpec((channels, chunk), columns),
            pl.BlockSpec((16, chunk), columns),
        ],
        out_specs=[
            pl.BlockSpec((channels, chunk), columns),
            pl.BlockSpec((tokens, channels), fixed),
        ],
        out_shape=[
            jax.ShapeDtypeStruct((channels, wide), jnp.bfloat16),
            jax.ShapeDtypeStruct((tokens, channels), jnp.float32),
        ],
        scratch_shapes=[
            pltpu.VMEM((items * (side + 2), side + 2 * INSET, chunk), jnp.float32),
            pltpu.VMEM((rims, chunk), jnp.float32),
            pltpu.VMEM((tokens, chunk), jnp.bfloat16),
        ],
        cost_estimate=pl.CostEstimate(
            flops=4 * tokens * channels * wide,
            bytes_accessed=4 * channels * wide * 2,
            transcendentals=0,
        ),
        name="ffn_back",
    )(d_filtered, rim, flipped, w_up, taps)


def shards(
    tokens, condition, counts, w_mod, w_qkv, w_out, w_up, w_down, conv_attn, conv_ffn, cotangent
):
    item_count, _, quad_rows, channels = tokens.shape
    half_side = math.isqrt(quad_rows)
    corner = lax.axis_index("narrow")
    row_half = corner // 2
    col_half = corner % 2
    living = (jnp.arange(item_count, dtype=jnp.int32) < counts[0]).astype(jnp.float32)[
        :, None, None, None
    ]
    start_map = tokens.reshape(item_count, half_side, half_side, channels).astype(jnp.float32)
    cond_f = condition.astype(jnp.float32)
    lifted = jax.nn.silu(cond_f).astype(jnp.bfloat16)
    all_lifted = wide_gather(lifted)
    modulation = jnp.dot(lifted, w_mod, preferred_element_type=jnp.float32).reshape(
        item_count, 6, channels
    )
    pieces = [modulation[:, place][:, None, None, :] for place in range(6)]
    shift_a, scale_a, gate_a, shift_f, scale_f, gate_f = pieces
    first_f, pull_attn_norm = jax.vjp(modulate, start_map, shift_a, scale_a)
    first_in = first_f.astype(jnp.bfloat16)
    padded_attn = extend(first_in, row_half, col_half, attn_across, attn_down)
    mixed_map = apply_taps(padded_attn, conv_attn, half_side, False).astype(jnp.bfloat16)
    groups = to_groups(mixed_map)
    queries, key_rows, values = split_heads(groups, w_qkv)
    scores = score(queries, key_rows)
    peak = jnp.max(scores, -1, keepdims=True)
    raised_exp = jnp.exp(scores - peak)
    summed = jnp.sum(raised_exp, -1, keepdims=True)
    attn_probs = (raised_exp / summed).astype(jnp.bfloat16)
    log_total = peak + jnp.log(summed)
    attended = jnp.einsum("ihqk,ikhe->iqhe", attn_probs, values, preferred_element_type=jnp.float32)
    attended = attended.astype(jnp.bfloat16).reshape(item_count, quad_rows, channels)
    returned = to_quads(attended)
    branch = jnp.dot(returned, w_out, preferred_element_type=jnp.float32)
    hidden_one = start_map + gate_a * branch
    second_f, pull_ffn_norm = jax.vjp(modulate, hidden_one, shift_f, scale_f)
    second = second_f.astype(jnp.bfloat16)
    token_count = item_count * quad_rows
    grad_res = (
        cotangent.reshape(item_count, half_side, half_side, channels).astype(jnp.float32) * living
    )
    d_branch_two = (grad_res * gate_f).astype(jnp.bfloat16)
    taps_ffn = jnp.pad(conv_ffn.astype(jnp.float32).T, ((0, 7), (0, 0)))
    flat_second = second.reshape(token_count, channels)
    branch_two, d_filtered, down_grad, tap_grad = ffn_pass(
        flat_second,
        rim_exchange(second, row_half, col_half).reshape(-1, channels),
        d_branch_two.reshape(token_count, channels),
        w_up,
        w_down,
        taps_ffn,
        item_count,
        half_side,
    )
    conv_ffn_grad = tap_grad[:9].T
    branch_two = branch_two.reshape(start_map.shape)
    output = ((hidden_one + gate_f * branch_two) * living).astype(jnp.bfloat16)
    d_gate_f = jnp.sum(grad_res * branch_two, (1, 2))
    d_filtered_map = d_filtered.reshape(item_count, half_side, half_side, -1)
    up_grad, d_second = ffn_back_pass(
        d_filtered,
        rim_exchange(d_filtered_map, row_half, col_half).reshape(-1, w_up.shape[1]),
        flat_second.T,
        w_up,
        taps_ffn,
        item_count,
        half_side,
    )
    d_second = d_second.reshape(start_map.shape)
    d_hidden_part, d_shift_f, d_scale_f = pull_ffn_norm(d_second)
    d_hidden = grad_res + d_hidden_part
    d_gate_a = jnp.sum(d_hidden * branch, (1, 2))
    d_branch = (d_hidden * gate_a).astype(jnp.bfloat16)
    proj_grad = jnp.einsum("ixyd,ixye->de", returned, d_branch, preferred_element_type=jnp.float32)
    d_returned = jnp.einsum(
        "ixye,de->ixyd", d_branch, w_out, preferred_element_type=jnp.float32
    ).astype(jnp.bfloat16)
    d_attended = to_groups(d_returned).reshape(item_count, quad_rows, HEADS, HEAD_DIM)
    queries, key_rows, values = split_heads(groups, w_qkv)
    scores = score(queries, key_rows)
    exact = jnp.exp(scores - log_total)
    rounded = exact.astype(jnp.bfloat16)
    d_probs = jnp.einsum("iqhe,ikhe->ihqk", d_attended, values, preferred_element_type=jnp.float32)
    d_values = jnp.einsum(
        "ihqk,iqhe->ikhe", rounded, d_attended, preferred_element_type=jnp.float32
    )
    d_scores = (exact * (d_probs - jnp.sum(d_probs * exact, -1, keepdims=True))).astype(
        jnp.bfloat16
    )
    d_queries = jnp.einsum(
        "ihqk,ikhe->iqhe", d_scores, key_rows, preferred_element_type=jnp.float32
    ) * HEAD_DIM ** (-0.5)
    d_keys = jnp.einsum(
        "ihqk,iqhe->ikhe", d_scores, queries, preferred_element_type=jnp.float32
    ) * HEAD_DIM ** (-0.5)
    d_triple = (
        jnp.stack([d_queries, d_keys, d_values], 2)
        .astype(jnp.bfloat16)
        .reshape(item_count, quad_rows, 3 * channels)
    )
    qkv_grad = jnp.einsum("iqd,iqe->de", groups, d_triple, preferred_element_type=jnp.float32)
    d_groups = jnp.einsum(
        "iqe,de->iqd", d_triple, w_qkv, preferred_element_type=jnp.float32
    ).astype(jnp.bfloat16)
    d_mixed = to_quads(d_groups)
    conv_attn_grad = tap_grads(padded_attn, d_mixed, half_side)
    d_padded_attn = extend(d_mixed, row_half, col_half, attn_across, attn_down)
    d_first = apply_taps(d_padded_attn, conv_attn, half_side, True).astype(jnp.bfloat16)
    d_start, d_shift_a, d_scale_a = pull_attn_norm(d_first.astype(jnp.float32))
    token_grad = (d_hidden + d_start).astype(jnp.bfloat16).reshape(tokens.shape)
    flat_parts = [
        d_shift_a.reshape(item_count, channels),
        d_scale_a.reshape(item_count, channels),
        d_gate_a,
        d_shift_f.reshape(item_count, channels),
        d_scale_f.reshape(item_count, channels),
        d_gate_f,
    ]
    d_modulation = jnp.stack(flat_parts, 1).reshape(item_count, 6 * channels)
    d_modulation = narrow_sum(d_modulation)
    _, silu_pull = jax.vjp(jax.nn.silu, cond_f)
    d_lifted = split_dot(d_modulation, w_mod, ((1,), (1,)))
    cond_grad = silu_pull(d_lifted)[0]
    all_modulation = wide_gather(d_modulation)
    block_rows = channels // (lax.axis_size("wide") * lax.axis_size("narrow"))
    own_block = lax.axis_index("wide") * lax.axis_size("narrow") + corner
    own_lifted = lax.dynamic_slice_in_dim(all_lifted, own_block * block_rows, block_rows, 1)
    mod_sum = split_dot(all_modulation, own_lifted, ((0,), (0,))).T
    blocks = lax.axis_size("wide") * lax.axis_size("narrow")
    up_blocks = up_grad.astype(jnp.bfloat16).reshape(blocks, -1, up_grad.shape[1])
    down_blocks = down_grad.astype(jnp.bfloat16).reshape(blocks, -1, channels)
    up_sum = halving_sum(up_blocks, 0)
    down_sum = halving_sum(down_blocks, 1)
    qkv_blocks = qkv_grad.astype(jnp.bfloat16).reshape(blocks, -1, 3 * channels)
    proj_blocks = proj_grad.astype(jnp.bfloat16).reshape(blocks, -1, channels)
    taps = jnp.concatenate([conv_attn_grad.reshape(blocks, -1), conv_ffn_grad.reshape(blocks, -1)], 1)
    rows = qkv_blocks.shape[1]
    taps_len = taps.shape[1]
    taps_wide = -(-taps_len // (rows * 128)) * 128
    taps = jnp.pad(taps, ((0, 0), (0, rows * taps_wide - taps_len)))
    taps = taps.astype(jnp.bfloat16).reshape(blocks, rows, taps_wide)
    left_sum = halving_sum(qkv_blocks[:, :, : 2 * channels], 0)
    right = jnp.concatenate([qkv_blocks[:, :, 2 * channels :], proj_blocks, taps], 2)
    right_sum = halving_sum(right, 1)
    qkv_sum = jnp.concatenate([left_sum, right_sum[:, :channels]], 1)
    proj_sum = right_sum[:, channels : 2 * channels]
    tap_sums = right_sum[:, 2 * channels :].reshape(-1)
    attn_len = conv_attn_grad.size // blocks
    conv_attn_sum = tap_sums[:attn_len].reshape(-1, 9)
    conv_ffn_sum = tap_sums[attn_len:taps_len].reshape(-1, 9)
    return (
        output.reshape(tokens.shape),
        token_grad,
        cond_grad,
        mod_sum,
        qkv_sum,
        proj_sum,
        up_sum,
        down_sum,
        conv_attn_sum,
        conv_ffn_sum,
    )


def solution(mesh):
    in_specs = (
        P("wide", "narrow", None, None),
        P("wide", None),
        P("wide"),
        P(),
        P(),
        P(),
        P(),
        P(),
        P(),
        P(),
        P("wide", "narrow", None, None),
    )
    out_specs = (
        P("wide", "narrow", None, None),
        P("wide", "narrow", None, None),
        P("wide", None),
        P(("wide", "narrow"), None),
        P(("wide", "narrow"), None),
        P(("wide", "narrow"), None),
        P(("wide", "narrow"), None),
        P(("wide", "narrow"), None),
        P(("wide", "narrow"), None),
        P(("wide", "narrow"), None),
    )
    return jax.shard_map(shards, mesh=mesh, in_specs=in_specs, out_specs=out_specs, check_vma=False)
```

```python
import functools
import math

import jax
import jax.numpy as jnp
from jax import lax
from jax.experimental import pallas as pl
from jax.experimental.pallas import tpu as pltpu
from jax.sharding import PartitionSpec as P

HEADS = 12
HEAD_DIM = 64


epsilon = 1e-06


def from_partner(shard, axis, bit):
    return lax.ppermute(shard, axis, [(i, i ^ 1 << bit) for i in range(lax.axis_size(axis))])


def normed(field_map):
    average = jnp.mean(field_map, -1, keepdims=True)
    centred = field_map - average
    variance = jnp.mean(centred * centred, -1, keepdims=True)
    return centred * lax.rsqrt(variance + epsilon)


def modulate(field_map, shift, scale):
    return normed(field_map) * (1.0 + scale) + shift


def attn_across(outgoing):
    return from_partner(outgoing, "narrow", 0)


def attn_down(outgoing):
    return from_partner(outgoing, "narrow", 1)


def extend(field_map, row_half, col_half, across, down):
    outgoing = jnp.where(col_half == 0, field_map[:, :, -1:], field_map[:, :, :1])
    incoming = across(outgoing)
    zeros_rim = jnp.zeros_like(incoming)
    left_rim = jnp.where(col_half == 1, incoming, zeros_rim)
    right_rim = jnp.where(col_half == 0, incoming, zeros_rim)
    widened = jnp.concatenate([left_rim, field_map, right_rim], 2)
    outgoing = jnp.where(row_half == 0, widened[:, -1:], widened[:, :1])
    incoming = down(outgoing)
    zeros_rim = jnp.zeros_like(incoming)
    top_rim = jnp.where(row_half == 1, incoming, zeros_rim)
    bottom_rim = jnp.where(row_half == 0, incoming, zeros_rim)
    return jnp.concatenate([top_rim, widened, bottom_rim], 1)


def apply_taps(padded, kernel, side_len, flipped):
    summed = jnp.zeros((padded.shape[0], side_len, side_len, padded.shape[3]), jnp.float32)
    weights_f = kernel.astype(jnp.float32)
    for stencil in range(9):
        row_off = stencil // 3
        col_off = stencil % 3
        if flipped:
            row_off = 2 - row_off
            col_off = 2 - col_off
        window = padded[:, row_off : row_off + side_len, col_off : col_off + side_len].astype(
            jnp.float32
        )
        summed = summed + window * weights_f[:, stencil]
    return summed


def tap_grads(padded, grad_map, side_len):
    grad_f = grad_map.astype(jnp.float32)
    columns = []
    for stencil in range(9):
        row_off = stencil // 3
        col_off = stencil % 3
        window = padded[:, row_off : row_off + side_len, col_off : col_off + side_len].astype(
            jnp.float32
        )
        columns.append(jnp.sum(window * grad_f, axis=(0, 1, 2)))
    return jnp.stack(columns, 1)


def to_groups(field_map):
    count, side_len, _, channels = field_map.shape
    quarter = side_len // 2
    pieces = field_map.reshape(count, quarter, 2, quarter, 2, channels).transpose(0, 2, 4, 1, 3, 5)
    pieces = pieces.reshape(count, 4, quarter * quarter, channels)
    incoming = lax.all_to_all(pieces, "narrow", split_axis=1, concat_axis=1, tiled=True)
    return incoming.reshape(count, 4 * quarter * quarter, channels)


def to_quads(group_rows):
    count, rows_all, channels = group_rows.shape
    pieces = group_rows.reshape(count, 4, rows_all // 4, channels)
    incoming = lax.all_to_all(pieces, "narrow", split_axis=1, concat_axis=1, tiled=True)
    quarter = math.isqrt(rows_all // 4)
    incoming = incoming.reshape(count, 2, 2, quarter, quarter, channels).transpose(0, 3, 1, 4, 2, 5)
    return incoming.reshape(count, 2 * quarter, 2 * quarter, channels)


def split_heads(groups, w_qkv):
    count, rows_all, _ = groups.shape
    triple = jnp.dot(groups, w_qkv, preferred_element_type=jnp.float32).astype(jnp.bfloat16)
    triple = triple.reshape(count, rows_all, 3, HEADS, HEAD_DIM)
    return (triple[:, :, 0], triple[:, :, 1], triple[:, :, 2])


def score(queries, key_rows):
    return jnp.einsum(
        "iqhe,ikhe->ihqk", queries, key_rows, preferred_element_type=jnp.float32
    ) * HEAD_DIM ** (-0.5)


def narrow_sum(part):
    for bit in range(lax.axis_size("narrow").bit_length() - 1):
        part = part + from_partner(part, "narrow", bit)
    return part


def wide_gather(block):
    count = lax.axis_size("wide")
    place = lax.axis_index("wide")
    held = block[None]
    for bit in range(count.bit_length() - 1):
        other = from_partner(held, "wide", bit)
        mine_high = (place >> bit) & 1
        low = jnp.where(mine_high == 1, other, held)
        high = jnp.where(mine_high == 1, held, other)
        held = jnp.concatenate([low, high], 0)
    return held.reshape((count * block.shape[0],) + block.shape[1:])


def split_dot(exact, coarse, dims):
    high = exact.astype(jnp.bfloat16)
    low = (exact - high.astype(jnp.float32)).astype(jnp.bfloat16)
    high_dot = lax.dot_general(high, coarse, (dims, ((), ())), preferred_element_type=jnp.float32)
    low_dot = lax.dot_general(low, coarse, (dims, ((), ())), preferred_element_type=jnp.float32)
    return high_dot + low_dot


def halving_sum(blocks, colour):
    wide_bits = lax.axis_size("wide").bit_length() - 1
    narrow_bits = lax.axis_size("narrow").bit_length() - 1
    order = [("narrow", 0)]
    first = [("wide", 0), ("narrow", 1)]
    order += first if colour == 0 else first[::-1]
    order += [("wide", bit) for bit in range(1, wide_bits)]
    names = [("wide", bit) for bit in range(wide_bits - 1, -1, -1)]
    names += [("narrow", bit) for bit in range(narrow_bits - 1, -1, -1)]
    held = blocks.reshape((2,) * len(names) + blocks.shape[1:])
    for step, (axis, bit) in enumerate(order):
        where = names.index((axis, bit))
        names.pop(where)
        mine = (lax.axis_index(axis) >> bit) & 1
        keep = lax.dynamic_index_in_dim(held, mine, where, keepdims=False)
        give = lax.dynamic_index_in_dim(held, 1 - mine, where, keepdims=False)
        got = from_partner(give, axis, bit)
        held = keep.astype(jnp.float32) + got.astype(jnp.float32)
        if step < len(order) - 1:
            held = held.astype(jnp.bfloat16)
    return held


LANES = 128
SUBLANES = 8
UNROLL = 4
GELU_SCALE = math.sqrt(2.0 / math.pi)
GELU_CUBE = 0.044715


def send_rims(column, row, point):
    size = lax.axis_size("narrow")
    column = lax.ppermute(column, "narrow", [(i, i ^ 1) for i in range(size)])
    row = lax.ppermute(row, "narrow", [(i, i ^ 2) for i in range(size)])
    point = lax.ppermute(point, "narrow", [(i, i ^ 3) for i in range(size)])
    channels = column.shape[-1]
    point = jnp.pad(point, ((0, 8 - point.shape[0]), (0, 0)))
    return column.reshape(-1, channels), row.reshape(-1, channels), point


def map_rims(field_map, row_half, col_half):
    items, side, _, channels = field_map.shape
    column = jnp.where(col_half == 0, field_map[:, :, -1], field_map[:, :, 0])
    row = jnp.where(row_half == 0, field_map[:, -1], field_map[:, 0])
    point = jnp.where(col_half == 0, row[:, -1], row[:, 0])
    column = column.reshape(items, side // 2, 2, channels).transpose(0, 2, 1, 3)
    return send_rims(column, row, point)


def woven_rims(woven, row_half, col_half):
    column = jnp.where(col_half == 0, woven[:, -1], woven[:, 0])
    row = jnp.where(row_half == 0, woven[:, :, -1], woven[:, :, 0])
    point = jnp.where(col_half == 0, row[:, -1], row[:, 0])
    return send_rims(column, row, point)


def weave(side):
    area = side * side
    place = lax.broadcasted_iota(jnp.int32, (area, area), 0)
    token = lax.broadcasted_iota(jnp.int32, (area, area), 1)
    column = place // side
    parity = (place % side) // (side // 2)
    source = (2 * (place % (side // 2)) + parity) * side + column
    return jnp.where(token == source, 1.0, 0.0).astype(jnp.bfloat16)


def weave_rows(target, source, items, side):
    area = side * side
    order = weave(side)
    for item in range(items):
        span = slice(item * area, (item + 1) * area)
        target[span, :] = jnp.dot(
            order, source[span, :], preferred_element_type=jnp.float32
        ).astype(jnp.bfloat16)


def unweave_rows(target, source, items, side):
    area = side * side
    order = weave(side)
    across = (((0,), (0,)), ((), ()))
    for item in range(items):
        span = slice(item * area, (item + 1) * area)
        exact = source[span, :]
        high = exact.astype(jnp.bfloat16)
        low = (exact - high.astype(jnp.float32)).astype(jnp.bfloat16)
        target[span, :] = lax.dot_general(
            order, high, across, preferred_element_type=jnp.float32
        ) + lax.dot_general(order, low, across, preferred_element_type=jnp.float32)


def fill_padded(padded, tile_of, column, row, point, upper, left, items, side):
    high = side + 2
    width = padded.shape[-1]
    right = 1.0 - left
    lower = 1.0 - upper
    where = lax.broadcasted_iota(jnp.int32, (SUBLANES, width), 0)

    def put(spot, tile, edge):
        even = tile[:SUBLANES]
        odd = tile[SUBLANES:]
        padded[spot, 0] = jnp.where(where == 0, edge * upper, pltpu.roll(odd, 1, 0))
        padded[spot, 1] = even
        padded[spot, 2] = odd
        padded[spot, 3] = jnp.where(
            where == SUBLANES - 1, edge * lower, pltpu.roll(even, SUBLANES - 1, 0)
        )

    for item in range(items):
        rim = column[item * side : (item + 1) * side]
        corner = point[item : item + 1]
        put(item * high, rim * left, corner * left)
        put(item * high + high - 1, rim * right, corner * right)

    def some_tiles(trip, carry):
        base = trip * UNROLL
        spot = base + 2 * (base // side) + 1
        for more in range(UNROLL):
            put(spot + more, tile_of(base + more), row[pl.ds(base + more, 1), :])
        return carry

    lax.fori_loop(0, items * side // UNROLL, some_tiles, 0)


def column_windows(padded, at, lanes):
    return [padded[at + tap % 3, tap // 3 : tap // 3 + 2, :, lanes] for tap in range(9)]


def summed_windows(windows, weights):
    parts = [windows[tap] * weights[tap] for tap in range(9)]
    while len(parts) > 1:
        joined = [parts[i] + parts[i + 1] for i in range(0, len(parts) - 1, 2)]
        parts = joined + parts[len(parts) - len(parts) % 2 :]
    return parts[0]


def as_wide(values):
    return values.astype(jnp.bfloat16).astype(jnp.float32)


def ffn_kernel(
    items,
    side,
    halves_ref,
    second_ref,
    column_ref,
    row_ref,
    point_ref,
    d_two_ref,
    w_up_ref,
    w_down_ref,
    taps_ref,
    two_ref,
    d_filtered_ref,
    down_ref,
    tap_grad_ref,
    padded,
    row,
    act,
    d_act,
    second,
    d_two,
    total,
):
    step = pl.program_id(0)
    chunk = w_up_ref.shape[1]
    low = jnp.bfloat16

    @pl.when(step == 0)
    def _():
        weave_rows(second, second_ref, items, side)
        weave_rows(d_two, d_two_ref, items, side)

    def raise_up(rows):
        return as_wide(jnp.dot(rows, w_up_ref[...], preferred_element_type=jnp.float32))

    def tile_of(number):
        return d_act[pl.ds(pl.multiple_of(number * side, side), side), :]

    d_act[...] = raise_up(second[...])
    row[...] = raise_up(row_ref[...])
    fill_padded(
        padded,
        tile_of,
        raise_up(column_ref[...]),
        row,
        raise_up(point_ref[...]),
        halves_ref[0],
        halves_ref[1],
        items,
        side,
    )
    d_act[...] = lax.dot_general(
        d_two[...], w_down_ref[...], (((1,), (1,)), ((), ())), preferred_element_type=jnp.float32
    )
    for lane in range(0, chunk, LANES):
        lanes = slice(lane, lane + LANES)
        weights = [taps_ref[tap : tap + 1, lanes] for tap in range(9)]

        def some_columns(trip, sums):
            base = trip * UNROLL
            corner = base + 2 * (base // side)
            for more in range(UNROLL):
                number = base + more
                start = corner + more
                at = pl.ds(pl.multiple_of(number * side, side), side)
                windows = column_windows(padded, start, lanes)
                v = summed_windows(windows, weights)
                square = v * v
                bend = jnp.tanh(GELU_SCALE * v * (1.0 + GELU_CUBE * square))
                half = 0.5 + 0.5 * bend
                act[at, lanes] = (v * half).reshape(side, LANES).astype(low)
                slope = half + 0.5 * v * (1.0 - bend * bend) * (
                    GELU_SCALE + (3.0 * GELU_CUBE * GELU_SCALE) * square
                )
                rounded = (d_act[at, lanes] * slope.reshape(side, LANES)).astype(low)
                d_filtered_ref[at, lanes] = rounded
                wide = rounded.astype(jnp.float32).reshape(2, SUBLANES, LANES)
                added = []
                for tap in range(9):
                    product = windows[tap] * wide
                    added.append(sums[tap] + (product[0] + product[1]))
                sums = tuple(added)
            return sums

        sums = tuple(jnp.zeros((SUBLANES, LANES), jnp.float32) for _ in range(9))
        sums = lax.fori_loop(0, items * side // UNROLL, some_columns, sums)
        for tap in range(9):
            tap_grad_ref[tap : tap + 1, lanes] = jnp.sum(sums[tap], 0, keepdims=True)
    tap_grad_ref[9:, :] = jnp.zeros((tap_grad_ref.shape[0] - 9, chunk), jnp.float32)
    down_ref[...] = lax.dot_general(
        act[...], d_two[...], (((0,), (0,)), ((), ())), preferred_element_type=jnp.float32
    ).astype(low)
    part = jnp.dot(act[...], w_down_ref[...], preferred_element_type=jnp.float32)

    @pl.when(step == 0)
    def _():
        total[...] = part

    @pl.when(step > 0)
    def _():
        total[...] += part

    @pl.when(step == pl.num_programs(0) - 1)
    def _():
        unweave_rows(two_ref, total, items, side)


def ffn_back_kernel(
    items,
    side,
    halves_ref,
    d_filtered_ref,
    column_ref,
    row_ref,
    point_ref,
    second_ref,
    w_up_ref,
    taps_ref,
    up_ref,
    d_second_ref,
    padded,
    row,
    d_raised,
    flipped,
    total,
):
    step = pl.program_id(0)
    chunk = w_up_ref.shape[1]
    low = jnp.bfloat16
    area = side * side

    @pl.when(step == 0)
    def _():
        order = weave(side)
        for item in range(items):
            span = slice(item * area, (item + 1) * area)
            flipped[:, span] = lax.dot_general(
                second_ref[span, :], order, (((0,), (1,)), ((), ())), preferred_element_type=jnp.float32
            ).astype(low)

    def tile_of(number):
        at = pl.ds(pl.multiple_of(number * side, side), side)
        return d_filtered_ref[at, :].astype(jnp.float32)

    row[...] = row_ref[...].astype(jnp.float32)
    fill_padded(
        padded,
        tile_of,
        column_ref[...].astype(jnp.float32),
        row,
        point_ref[...].astype(jnp.float32),
        halves_ref[0],
        halves_ref[1],
        items,
        side,
    )
    for lane in range(0, chunk, LANES):
        lanes = slice(lane, lane + LANES)
        weights = [taps_ref[8 - tap : 9 - tap, lanes] for tap in range(9)]

        def some_columns(trip, carry):
            base = trip * UNROLL
            corner = base + 2 * (base // side)
            for more in range(UNROLL):
                number = base + more
                start = corner + more
                at = pl.ds(pl.multiple_of(number * side, side), side)
                v = summed_windows(column_windows(padded, start, lanes), weights)
                d_raised[at, lanes] = v.reshape(side, LANES).astype(low)
            return carry

        lax.fori_loop(0, items * side // UNROLL, some_columns, 0)
    up_ref[...] = jnp.dot(flipped[...], d_raised[...], preferred_element_type=jnp.float32).astype(
        low
    )
    part = lax.dot_general(
        d_raised[...], w_up_ref[...], (((1,), (1,)), ((), ())), preferred_element_type=jnp.float32
    )

    @pl.when(step == 0)
    def _():
        total[...] = part

    @pl.when(step > 0)
    def _():
        total[...] += part

    @pl.when(step == pl.num_programs(0) - 1)
    def _():
        unweave_rows(d_second_ref, total, items, side)


def padded_shape(items, side, chunk):
    return pltpu.VMEM((items * (side + 2), 4, SUBLANES, chunk), jnp.float32)


def ffn_pass(halves, second, rims, d_two, w_up, w_down, taps, items, side, chunk=256):
    tokens, channels = second.shape
    wide = w_up.shape[1]
    fixed = lambda step: (0, 0)
    columns = lambda step: (0, step)
    rows = lambda step: (step, 0)
    return pl.pallas_call(
        functools.partial(ffn_kernel, items, side),
        grid=(wide // chunk,),
        in_specs=[
            pl.BlockSpec(memory_space=pltpu.SMEM),
            pl.BlockSpec((tokens, channels), fixed),
            pl.BlockSpec(rims[0].shape, fixed),
            pl.BlockSpec(rims[1].shape, fixed),
            pl.BlockSpec(rims[2].shape, fixed),
            pl.BlockSpec((tokens, channels), fixed),
            pl.BlockSpec((channels, chunk), columns),
            pl.BlockSpec((chunk, channels), rows),
            pl.BlockSpec((16, chunk), columns),
        ],
        out_specs=[
            pl.BlockSpec((tokens, channels), fixed),
            pl.BlockSpec((tokens, chunk), columns),
            pl.BlockSpec((chunk, channels), rows),
            pl.BlockSpec((16, chunk), columns),
        ],
        out_shape=[
            jax.ShapeDtypeStruct((tokens, channels), jnp.float32),
            jax.ShapeDtypeStruct((tokens, wide), jnp.bfloat16),
            jax.ShapeDtypeStruct((wide, channels), jnp.bfloat16),
            jax.ShapeDtypeStruct((16, wide), jnp.float32),
        ],
        scratch_shapes=[
            padded_shape(items, side, chunk),
            pltpu.VMEM((items * side, chunk), jnp.float32),
            pltpu.VMEM((tokens, chunk), jnp.bfloat16),
            pltpu.VMEM((tokens, chunk), jnp.float32),
            pltpu.VMEM((tokens, channels), jnp.bfloat16),
            pltpu.VMEM((tokens, channels), jnp.bfloat16),
            pltpu.VMEM((tokens, channels), jnp.float32),
        ],
        cost_estimate=pl.CostEstimate(
            flops=8 * tokens * channels * wide,
            bytes_accessed=4 * channels * wide * 4,
            transcendentals=tokens * wide,
        ),
        name="ffn",
    )(halves, second, *rims, d_two, w_up, w_down, taps)


def ffn_back_pass(halves, d_filtered, rims, second, w_up, taps, items, side, chunk=256):
    tokens, wide = d_filtered.shape
    channels = w_up.shape[0]
    fixed = lambda step: (0, 0)
    columns = lambda step: (0, step)
    return pl.pallas_call(
        functools.partial(ffn_back_kernel, items, side),
        grid=(wide // chunk,),
        in_specs=[
            pl.BlockSpec(memory_space=pltpu.SMEM),
            pl.BlockSpec((tokens, chunk), columns),
            pl.BlockSpec((rims[0].shape[0], chunk), columns),
            pl.BlockSpec((rims[1].shape[0], chunk), columns),
            pl.BlockSpec((rims[2].shape[0], chunk), columns),
            pl.BlockSpec((tokens, channels), fixed),
            pl.BlockSpec((channels, chunk), columns),
            pl.BlockSpec((16, chunk), columns),
        ],
        out_specs=[
            pl.BlockSpec((channels, chunk), columns),
            pl.BlockSpec((tokens, channels), fixed),
        ],
        out_shape=[
            jax.ShapeDtypeStruct((channels, wide), jnp.bfloat16),
            jax.ShapeDtypeStruct((tokens, channels), jnp.float32),
        ],
        scratch_shapes=[
            padded_shape(items, side, chunk),
            pltpu.VMEM((items * side, chunk), jnp.float32),
            pltpu.VMEM((tokens, chunk), jnp.bfloat16),
            pltpu.VMEM((channels, tokens), jnp.bfloat16),
            pltpu.VMEM((tokens, channels), jnp.float32),
        ],
        cost_estimate=pl.CostEstimate(
            flops=4 * tokens * channels * wide,
            bytes_accessed=4 * channels * wide * 2,
            transcendentals=0,
        ),
        name="ffn_back",
    )(halves, d_filtered, *rims, second, w_up, taps)


def shards(
    tokens, condition, counts, w_mod, w_qkv, w_out, w_up, w_down, conv_attn, conv_ffn, cotangent
):
    item_count, _, quad_rows, channels = tokens.shape
    half_side = math.isqrt(quad_rows)
    corner = lax.axis_index("narrow")
    row_half = corner // 2
    col_half = corner % 2
    living = (jnp.arange(item_count, dtype=jnp.int32) < counts[0]).astype(jnp.float32)[
        :, None, None, None
    ]
    start_map = tokens.reshape(item_count, half_side, half_side, channels).astype(jnp.float32)
    cond_f = condition.astype(jnp.float32)
    lifted = jax.nn.silu(cond_f).astype(jnp.bfloat16)
    all_lifted = wide_gather(lifted)
    modulation = jnp.dot(lifted, w_mod, preferred_element_type=jnp.float32).reshape(
        item_count, 6, channels
    )
    pieces = [modulation[:, place][:, None, None, :] for place in range(6)]
    shift_a, scale_a, gate_a, shift_f, scale_f, gate_f = pieces
    first_f, pull_attn_norm = jax.vjp(modulate, start_map, shift_a, scale_a)
    first_in = first_f.astype(jnp.bfloat16)
    padded_attn = extend(first_in, row_half, col_half, attn_across, attn_down)
    mixed_map = apply_taps(padded_attn, conv_attn, half_side, False).astype(jnp.bfloat16)
    groups = to_groups(mixed_map)
    queries, key_rows, values = split_heads(groups, w_qkv)
    scores = score(queries, key_rows)
    peak = jnp.max(scores, -1, keepdims=True)
    raised_exp = jnp.exp(scores - peak)
    summed = jnp.sum(raised_exp, -1, keepdims=True)
    attn_probs = (raised_exp / summed).astype(jnp.bfloat16)
    log_total = peak + jnp.log(summed)
    attended = jnp.einsum("ihqk,ikhe->iqhe", attn_probs, values, preferred_element_type=jnp.float32)
    attended = attended.astype(jnp.bfloat16).reshape(item_count, quad_rows, channels)
    returned = to_quads(attended)
    branch = jnp.dot(returned, w_out, preferred_element_type=jnp.float32)
    hidden_one = start_map + gate_a * branch
    second_f, pull_ffn_norm = jax.vjp(modulate, hidden_one, shift_f, scale_f)
    second = second_f.astype(jnp.bfloat16)
    token_count = item_count * quad_rows
    grad_res = (
        cotangent.reshape(item_count, half_side, half_side, channels).astype(jnp.float32) * living
    )
    d_branch_two = (grad_res * gate_f).astype(jnp.bfloat16)
    taps_ffn = jnp.pad(conv_ffn.astype(jnp.float32).T, ((0, 7), (0, 0)))
    flat_second = second.reshape(token_count, channels)
    halves = jnp.stack([row_half, col_half]).astype(jnp.float32)
    branch_two, d_filtered, down_grad, tap_grad = ffn_pass(
        halves,
        flat_second,
        map_rims(second, row_half, col_half),
        d_branch_two.reshape(token_count, channels),
        w_up,
        w_down,
        taps_ffn,
        item_count,
        half_side,
    )
    conv_ffn_grad = tap_grad[:9].T
    branch_two = branch_two.reshape(start_map.shape)
    output = ((hidden_one + gate_f * branch_two) * living).astype(jnp.bfloat16)
    d_gate_f = jnp.sum(grad_res * branch_two, (1, 2))
    d_filtered_map = d_filtered.reshape(item_count, half_side, half_side, -1)
    up_grad, d_second = ffn_back_pass(
        halves,
        d_filtered,
        woven_rims(d_filtered_map, row_half, col_half),
        flat_second,
        w_up,
        taps_ffn,
        item_count,
        half_side,
    )
    d_second = d_second.reshape(start_map.shape)
    d_hidden_part, d_shift_f, d_scale_f = pull_ffn_norm(d_second)
    d_hidden = grad_res + d_hidden_part
    d_gate_a = jnp.sum(d_hidden * branch, (1, 2))
    d_branch = (d_hidden * gate_a).astype(jnp.bfloat16)
    proj_grad = jnp.einsum("ixyd,ixye->de", returned, d_branch, preferred_element_type=jnp.float32)
    d_returned = jnp.einsum(
        "ixye,de->ixyd", d_branch, w_out, preferred_element_type=jnp.float32
    ).astype(jnp.bfloat16)
    d_attended = to_groups(d_returned).reshape(item_count, quad_rows, HEADS, HEAD_DIM)
    queries, key_rows, values = split_heads(groups, w_qkv)
    scores = score(queries, key_rows)
    exact = jnp.exp(scores - log_total)
    rounded = exact.astype(jnp.bfloat16)
    d_probs = jnp.einsum("iqhe,ikhe->ihqk", d_attended, values, preferred_element_type=jnp.float32)
    d_values = jnp.einsum(
        "ihqk,iqhe->ikhe", rounded, d_attended, preferred_element_type=jnp.float32
    )
    d_scores = (exact * (d_probs - jnp.sum(d_probs * exact, -1, keepdims=True))).astype(
        jnp.bfloat16
    )
    d_queries = jnp.einsum(
        "ihqk,ikhe->iqhe", d_scores, key_rows, preferred_element_type=jnp.float32
    ) * HEAD_DIM ** (-0.5)
    d_keys = jnp.einsum(
        "ihqk,iqhe->ikhe", d_scores, queries, preferred_element_type=jnp.float32
    ) * HEAD_DIM ** (-0.5)
    d_triple = (
        jnp.stack([d_queries, d_keys, d_values], 2)
        .astype(jnp.bfloat16)
        .reshape(item_count, quad_rows, 3 * channels)
    )
    qkv_grad = jnp.einsum("iqd,iqe->de", groups, d_triple, preferred_element_type=jnp.float32)
    d_groups = jnp.einsum(
        "iqe,de->iqd", d_triple, w_qkv, preferred_element_type=jnp.float32
    ).astype(jnp.bfloat16)
    d_mixed = to_quads(d_groups)
    conv_attn_grad = tap_grads(padded_attn, d_mixed, half_side)
    d_padded_attn = extend(d_mixed, row_half, col_half, attn_across, attn_down)
    d_first = apply_taps(d_padded_attn, conv_attn, half_side, True).astype(jnp.bfloat16)
    d_start, d_shift_a, d_scale_a = pull_attn_norm(d_first.astype(jnp.float32))
    token_grad = (d_hidden + d_start).astype(jnp.bfloat16).reshape(tokens.shape)
    flat_parts = [
        d_shift_a.reshape(item_count, channels),
        d_scale_a.reshape(item_count, channels),
        d_gate_a,
        d_shift_f.reshape(item_count, channels),
        d_scale_f.reshape(item_count, channels),
        d_gate_f,
    ]
    d_modulation = jnp.stack(flat_parts, 1).reshape(item_count, 6 * channels)
    d_modulation = narrow_sum(d_modulation)
    _, silu_pull = jax.vjp(jax.nn.silu, cond_f)
    d_lifted = split_dot(d_modulation, w_mod, ((1,), (1,)))
    cond_grad = silu_pull(d_lifted)[0]
    all_modulation = wide_gather(d_modulation)
    block_rows = channels // (lax.axis_size("wide") * lax.axis_size("narrow"))
    own_block = lax.axis_index("wide") * lax.axis_size("narrow") + corner
    own_lifted = lax.dynamic_slice_in_dim(all_lifted, own_block * block_rows, block_rows, 1)
    mod_sum = split_dot(all_modulation, own_lifted, ((0,), (0,))).T
    blocks = lax.axis_size("wide") * lax.axis_size("narrow")
    up_blocks = up_grad.astype(jnp.bfloat16).reshape(blocks, -1, up_grad.shape[1])
    down_blocks = down_grad.astype(jnp.bfloat16).reshape(blocks, -1, channels)
    up_sum = halving_sum(up_blocks, 0)
    down_sum = halving_sum(down_blocks, 1)
    qkv_blocks = qkv_grad.astype(jnp.bfloat16).reshape(blocks, -1, 3 * channels)
    proj_blocks = proj_grad.astype(jnp.bfloat16).reshape(blocks, -1, channels)
    taps = jnp.concatenate([conv_attn_grad.reshape(blocks, -1), conv_ffn_grad.reshape(blocks, -1)], 1)
    rows = qkv_blocks.shape[1]
    taps_len = taps.shape[1]
    taps_wide = -(-taps_len // (rows * 128)) * 128
    taps = jnp.pad(taps, ((0, 0), (0, rows * taps_wide - taps_len)))
    taps = taps.astype(jnp.bfloat16).reshape(blocks, rows, taps_wide)
    left_sum = halving_sum(qkv_blocks[:, :, : 2 * channels], 0)
    right = jnp.concatenate([qkv_blocks[:, :, 2 * channels :], proj_blocks, taps], 2)
    right_sum = halving_sum(right, 1)
    qkv_sum = jnp.concatenate([left_sum, right_sum[:, :channels]], 1)
    proj_sum = right_sum[:, channels : 2 * channels]
    tap_sums = right_sum[:, 2 * channels :].reshape(-1)
    attn_len = conv_attn_grad.size // blocks
    conv_attn_sum = tap_sums[:attn_len].reshape(-1, 9)
    conv_ffn_sum = tap_sums[attn_len:taps_len].reshape(-1, 9)
    return (
        output.reshape(tokens.shape),
        token_grad,
        cond_grad,
        mod_sum,
        qkv_sum,
        proj_sum,
        up_sum,
        down_sum,
        conv_attn_sum,
        conv_ffn_sum,
    )


def solution(mesh):
    in_specs = (
        P("wide", "narrow", None, None),
        P("wide", None),
        P("wide"),
        P(),
        P(),
        P(),
        P(),
        P(),
        P(),
        P(),
        P("wide", "narrow", None, None),
    )
    out_specs = (
        P("wide", "narrow", None, None),
        P("wide", "narrow", None, None),
        P("wide", None),
        P(("wide", "narrow"), None),
        P(("wide", "narrow"), None),
        P(("wide", "narrow"), None),
        P(("wide", "narrow"), None),
        P(("wide", "narrow"), None),
        P(("wide", "narrow"), None),
        P(("wide", "narrow"), None),
    )
    return jax.shard_map(shards, mesh=mesh, in_specs=in_specs, out_specs=out_specs, check_vma=False)
```
